32 devices in a mesh: seq: 8 (over y, x, core), head: 4 (over z).
Axes of the slice: x: 2, y: 2, z: 4, core: 2. Of those that a mesh axis runs over, the one named last changes fastest.
Arguments:
- text_states: bfloat16 [2048, 4096], P('seq', 'head'), may hold values from -200 to 200
- query_weight: bfloat16 [4096, 4096], P(None, 'head'), may hold values from -0.09375 to 0.09375
- image_keys: bfloat16 [4096, 1024], P('seq', 'head'), may hold values from -12 to 12
- image_values: bfloat16 [4096, 1024], P('seq', 'head'), may hold values from -24 to 24
- output_weight: bfloat16 [4096, 4096], P('head'), may hold values from -0.09375 to 0.09375
- attn_gate: float32 [1], replicated, may hold values from 0.3 to 1.5
- frame_lengths: int32 [16], replicated, may hold values from 1 to 512, 4096 in all
- frame_limit: int32 [32], replicated, may hold values from 0 to 16
Outputs:
- gated_branch: bfloat16 [2048, 4096], P('seq', 'head')
The draws below stay inside these ranges and needn't reach their ends.
Inputs may be any that keep to these rules, and one draw needn't show every extreme that they name: `frame_lengths`: the lengths sum to 4096.
All inputs are finite; a program needn't handle non-finite values.
Results may differ from the reference program's by a relative error of at most 0.014.
The reference program's roundings to bfloat16 on the way count: a program that leaves them out, or rounds other values in their place, can miss the bound.
Values may be sent and summed in bfloat16 or wider, within the bound.
A program may use at most 128 MiB of HBM per device.

```python
import math
import jax
import jax.numpy as jnp
import numpy as np
from jax import lax

D = 4096
HEADS = 32
KV_HEADS = 8
HD = 128
VID_DEV = 512
TBLK = 64
GROUP = 4
TEXT = 2048
VIDEO = 4096
FRAMES = 16
TEXT_BLOCKS = 32


def draw_text_states(key, part):
    normal_draw = jax.random.normal(jax.random.fold_in(key, 11), (TEXT, D), jnp.float32)
    return jnp.clip(normal_draw, -200.0, 200.0).astype(jnp.bfloat16)


def touch_ends(drawn, stream_key, low, largest):
    spot = [jax.random.randint(jax.random.fold_in(stream_key, axis), (), 0, length) for axis, length in enumerate(drawn.shape)]
    widest = drawn.shape.index(max(drawn.shape))
    beside = spot[:widest] + [(spot[widest] + 1) % drawn.shape[widest]] + spot[widest + 1:]
    return drawn.at[tuple(spot)].set(low).at[tuple(beside)].set(largest)


def block_scale(stream_key, extent, split, smallest, largest):
    def one(position, blocks):
        heights = jax.random.uniform(jax.random.fold_in(jax.random.fold_in(stream_key, 6), position), (blocks,), jnp.float32, smallest / len(split), largest / len(split))
        return jnp.repeat(jnp.exp(heights), extent[position] // blocks).reshape((-1,) + (1,) * (len(extent) - position - 1))

    factor_of = one(*split[0])
    for cut in split[1:]:
        factor_of = factor_of * one(*cut)
    return factor_of


def length_profile(count, total, reach, lean):
    loads = [(1 << 20) // math.isqrt(standing ** lean) + 1 for standing in range(2, count + 1)]
    rest, given = total - reach - (count - 1), [1] * (count - 1)
    while rest > 0:
        free = [i for i in range(count - 1) if given[i] < reach]
        whole, remaining = sum([loads[i] for i in free]), rest
        for i in free:
            addition = min(reach - given[i], max(1, remaining * loads[i] // whole), rest)
            given[i] = given[i] + addition
            rest = rest - addition
    return np.array([reach] + given)


def uneven(rng, count, total, limit, slope):
    if count == 2:
        one = jax.random.randint(rng, (), max(1, total - limit), min(limit, total - 1) + 1)
        return jnp.stack([one, total - one])
    sizes = jnp.asarray(length_profile(count, total, limit, slope), jnp.int32)
    couples = (count - 1) // 2
    giver, sink = sizes[1:1 + 2 * couples:2], sizes[2:2 + 2 * couples:2]
    margin = jnp.minimum(giver - 1, limit - sink)
    moved = jax.random.randint(jax.random.fold_in(rng, 1), (couples,), 0, 1 << 20) % (margin + 1)
    sizes = sizes.at[1:1 + 2 * couples:2].set(giver - moved).at[2:2 + 2 * couples:2].set(sink + moved)
    return sizes[jax.random.permutation(jax.random.fold_in(rng, 2), count)]


def centred(stream_key, extent, scale, reach, cuts=(), held_as=jnp.bfloat16):
    factor_of = block_scale(stream_key, extent, cuts, -0.22, 0.18) if cuts else 1.0
    drawn = jax.random.normal(stream_key, extent, jnp.float32) * scale * factor_of
    return jnp.minimum(jnp.maximum(drawn, -reach), reach).astype(held_as)


def setup_inputs(seed: int = 0) -> dict:
    keys = jax.random.split(jax.random.key(seed), 9)
    return {
        "text_states": draw_text_states(jax.random.fold_in(keys[8], 71), 0),
        "query_weight": centred(keys[1], (D, HEADS * HD), D ** -0.5, 0.09375, ((1, 4),)),
        "image_keys": centred(keys[2], (VIDEO, KV_HEADS * HD), 2.0, 12.0, ((0, 8), (1, 4))),
        "image_values": centred(keys[3], (VIDEO, KV_HEADS * HD), 4.0, 24.0, ((0, 8), (1, 4))),
        "output_weight": centred(keys[4], (HEADS * HD, D), (HEADS * HD) ** -0.5, 0.09375, ((0, 4),)),
        "attn_gate": jnp.clip(jax.random.uniform(keys[5], (1,), jnp.float32, 0.3, 1.5), 0.3, 1.5),
        "frame_lengths": uneven(keys[6], FRAMES, VIDEO, VID_DEV, 2).astype(jnp.int32),
        "frame_limit": touch_ends(jax.random.randint(keys[7], (TEXT_BLOCKS,), 0, FRAMES + 1), jax.random.fold_in(keys[7], 1), 0, FRAMES).astype(jnp.int32),
    }


masked_fill = -1e+30

def reference(text_states, query_weight, image_keys, image_values, output_weight, attn_gate, frame_lengths, frame_limit):
    queries = jnp.dot(text_states, query_weight, preferred_element_type=jnp.float32).astype(jnp.bfloat16)
    frame_ends = jnp.cumsum(frame_lengths).astype(jnp.int32)
    token_positions = jnp.arange(VIDEO, dtype=jnp.int32)
    key_frames = lax.optimization_barrier(jnp.sum((frame_ends[None, :] <= token_positions[:, None]).astype(jnp.int32), axis=1))
    row_limits = jnp.repeat(frame_limit, TBLK)
    query_heads = queries.reshape(TEXT, HEADS, HD).transpose(1, 0, 2)
    key_head_count = image_keys.reshape(VIDEO, KV_HEADS, HD).transpose(1, 0, 2)
    value_heads = image_values.reshape(VIDEO, KV_HEADS, HD).transpose(1, 0, 2)
    score_scale = 1.0 / math.sqrt(HD)
    block_rows = TEXT // 4

    def one_block(head_no, block_no):
        head_rows = lax.dynamic_index_in_dim(query_heads, head_no, 0, keepdims=False)
        query_rows = lax.dynamic_slice_in_dim(head_rows, block_no * block_rows, block_rows, 0)
        key_rows = lax.dynamic_index_in_dim(key_head_count, head_no // GROUP, 0, keepdims=False)
        value_rows = lax.dynamic_index_in_dim(value_heads, head_no // GROUP, 0, keepdims=False)
        limits = lax.dynamic_slice_in_dim(row_limits, block_no * block_rows, block_rows, 0)
        scores = jnp.dot(query_rows, key_rows.T, preferred_element_type=jnp.float32) * score_scale
        visible = key_frames[None, :] < limits[:, None]
        best_score = lax.optimization_barrier(jnp.max(jnp.where(visible, scores, masked_fill), axis=1))
        weights = jnp.where(visible, jnp.exp(scores - best_score[:, None]), 0.0)
        weight_sum = lax.optimization_barrier(jnp.sum(weights, axis=1))
        mixed = jnp.dot(weights.astype(jnp.bfloat16), value_rows, preferred_element_type=jnp.float32)
        return (mixed / jnp.maximum(weight_sum, 1.0)[:, None]).astype(jnp.bfloat16)

    def one_head(head_no):
        blocks = lax.map(lambda block_no: one_block(head_no, block_no), jnp.arange(4, dtype=jnp.int32))
        return blocks.reshape(TEXT, HD)
    heads_out = lax.map(one_head, jnp.arange(HEADS, dtype=jnp.int32))
    attention_output = heads_out.transpose(1, 0, 2).reshape(TEXT, HEADS * HD)
    projected = jnp.dot(attention_output, output_weight, preferred_element_type=jnp.float32)
    return (jnp.tanh(attn_gate[0]) * projected).astype(jnp.bfloat16)
```

```python
import functools
import math

import jax
import jax.numpy as jnp
from jax import lax
from jax.experimental import pallas as pl
from jax.experimental.pallas import tpu as pltpu
from jax.sharding import PartitionSpec as P

HD = 128
TBLK = 64
GROUP = 4
SUPER = 4096
LOW = -1e30


def kernel(
    n, p, text, wq_hbm, k_hbm, v_hbm, wo_hbm, gate, lengths, limits, out,
    tbuf, wq, wo, kbuf, vbuf, qbuf, abuf, scores, pbuf, sbuf, rup, rdn,
    local_sem, t_recv, t_up, t_dn, r_up, r_dn, r_send, k_recv, k_send, v_recv, v_send,
):
    s = lax.axis_index("seq")
    z = lax.axis_index("head")
    rows, feat = text.shape
    chunks = rows // TBLK
    vid = k_hbm.shape[0]
    local_kv = k_hbm.shape[1] // HD
    bits = n.bit_length() - 1

    def flip(index, mask):
        for b in range(bits):
            bit = 1 << b
            if mask & bit:
                index = index + bit - 2 * bit * ((index // bit) % 2)
        return index

    key_order = [*range(1, bits), 0]
    value_order = [*range(2, bits), 1, 0] if bits > 1 else [0]

    barrier = pltpu.get_barrier_semaphore()
    has_up, has_dn = z < p - 1, z > 0
    for b in range(bits):
        pl.semaphore_signal(barrier, inc=1, device_id={"seq": flip(s, 1 << b)})

    @pl.when(has_up)
    def _():
        pl.semaphore_signal(barrier, inc=1, device_id={"head": z + 1})

    @pl.when(has_dn)
    def _():
        pl.semaphore_signal(barrier, inc=1, device_id={"head": z - 1})

    local = [
        pltpu.make_async_copy(text, tbuf.at[z], local_sem.at[0]),
        pltpu.make_async_copy(wq_hbm, wq, local_sem.at[1]),
        pltpu.make_async_copy(k_hbm, kbuf.at[s], local_sem.at[2]),
        pltpu.make_async_copy(v_hbm, vbuf.at[s], local_sem.at[3]),
        pltpu.make_async_copy(wo_hbm, wo, local_sem.at[4]),
    ]
    for copy in local:
        copy.start()
    peers = bits + jnp.where(has_up, 1, 0) + jnp.where(has_dn, 1, 0)
    pl.semaphore_wait(barrier, peers)

    def span(c):
        return pl.ds(pl.multiple_of(c * TBLK, TBLK), TBLK)

    def text_copy(c, source, up, own=False):
        block = tbuf.at[source, span(c)]
        return pltpu.make_async_remote_copy(
            src_ref=text.at[span(c)] if own else block,
            dst_ref=block,
            send_sem=(t_up if up else t_dn).at[c * p + source],
            recv_sem=t_recv.at[c * p + source],
            device_id={"head": z + 1 if up else z - 1},
        )

    def text_own(c):
        @pl.when(has_up)
        def _():
            text_copy(c, z, True, True).start()

        @pl.when(has_dn)
        def _():
            text_copy(c, z, False, True).start()

    def text_hop(c, d):
        @pl.when(z - d >= 0)
        def _():
            text_copy(c, z - d, True).wait_recv()

            @pl.when(has_up)
            def _():
                text_copy(c, z - d, True).start()

        @pl.when(z + d < p)
        def _():
            text_copy(c, z + d, False).wait_recv()

            @pl.when(has_dn)
            def _():
                text_copy(c, z + d, False).start()

    def kv_copy(keys, mask, b):
        buf, hbm = (kbuf, k_hbm) if keys else (vbuf, v_hbm)
        recv, send = (k_recv, k_send) if keys else (v_recv, v_send)
        block = buf.at[flip(s, mask)]
        return pltpu.make_async_remote_copy(
            src_ref=hbm if mask == 0 else block,
            dst_ref=block,
            send_sem=send.at[mask | (1 << b)],
            recv_sem=recv.at[mask | (1 << b)],
            device_id={"seq": flip(s, 1 << b)},
        )

    def kv_send(keys, mask, step):
        order = key_order if keys else value_order
        for b in order[step:]:
            kv_copy(keys, mask, b).start()

    def kv_wait(keys, mask):
        buf, recv, send = (kbuf, k_recv, k_send) if keys else (vbuf, v_recv, v_send)
        block = buf.at[flip(s, mask)]
        pltpu.make_async_remote_copy(
            src_ref=block, dst_ref=block, send_sem=send.at[mask], recv_sem=recv.at[mask],
            device_id={"seq": flip(s, 1)},
        ).wait_recv()

    def masks_before(order, step):
        masks = [0]
        for b in order[:step]:
            masks = masks + [m | (1 << b) for m in masks]
        return masks

    def kv_step(step):
        for m_index in range(1 << step):
            for keys, order in ((True, key_order), (False, value_order)):
                mask = masks_before(order, step)[m_index] | (1 << order[step])
                kv_wait(keys, mask)
                kv_send(keys, mask, step + 1)

    def sum_copy(c, d, up):
        return pltpu.make_async_remote_copy(
            src_ref=sbuf.at[c * p + d],
            dst_ref=(rup if up else rdn).at[c * p + d],
            send_sem=r_send.at[c * p + d],
            recv_sem=(r_up if up else r_dn).at[c * p + d],
            device_id={"head": z + 1 if up else z - 1},
        )

    def sum_hop(c, h):
        for d in reversed(range(p)):
            @pl.when((z == h) & (z < d))
            def _():
                sum_copy(c, d, True).wait_recv()
                i = c * p + d
                sbuf[i] = (pbuf[i] + rup[i].astype(jnp.float32)).astype(jnp.bfloat16)
                sum_copy(c, d, True).start()
        for d in range(p):
            @pl.when((p - 1 - z == h) & (d < z))
            def _():
                sum_copy(c, d, False).wait_recv()
                i = c * p + d
                sbuf[i] = (pbuf[i] + rdn[i].astype(jnp.float32)).astype(jnp.bfloat16)
                sum_copy(c, d, False).start()

    def sum_last(c):
        i = c * p + z

        @pl.when(has_dn)
        def _():
            sum_copy(c, z, True).wait_recv()
            pbuf[i] = pbuf[i] + rup[i].astype(jnp.float32)

        @pl.when(has_up)
        def _():
            sum_copy(c, z, False).wait_recv()
            pbuf[i] = pbuf[i] + rdn[i].astype(jnp.float32)

        factor = jnp.tanh(jnp.full((1, out.shape[1]), gate[0], jnp.float32))
        out[span(c), :] = (factor * pbuf[i]).astype(jnp.bfloat16)

    def project(c):
        wide = 256

        def tile(j, carry):
            cols = pl.ds(pl.multiple_of(j * wide, wide), wide)
            total = jnp.zeros((TBLK, wide), jnp.float32)
            for source in range(p):
                total += jnp.dot(
                    tbuf[source, span(c), :], wq[source * feat : (source + 1) * feat, cols],
                    preferred_element_type=jnp.float32,
                )
            qbuf[:, cols] = total.astype(jnp.bfloat16)
            return carry

        lax.fori_loop(0, qbuf.shape[1] // wide, tile, 0)

    per = min(n, max(1, SUPER // vid))
    score_scale = math.log2(math.e) / math.sqrt(HD)

    def head_cols(h):
        return pl.ds(pl.multiple_of(h * HD, HD), HD)

    def visible_tokens(c):
        limit = limits[s * chunks + c]
        total = jnp.int32(0)
        for f in range(lengths.shape[0]):
            total += jnp.where(f < limit, lengths[f], 0)
        return total

    def attend(c, h, seen):
        q = jnp.concatenate([qbuf[:, head_cols(h * GROUP + g)] for g in range(GROUP)], axis=0)
        m_rows = GROUP * TBLK

        def lanes(x, op):
            parts = [x[:, i * HD : (i + 1) * HD] for i in range(x.shape[1] // HD)]
            return functools.reduce(op, parts)

        def part(u, state):
            best, weight, acc = state
            wide = jnp.full((m_rows, HD), LOW, jnp.float32)
            for i in range(per):
                block = u * per + i
                x = lax.dot_general(
                    q, kbuf[block, :, head_cols(h)], (((1,), (1,)), ((), ())),
                    preferred_element_type=jnp.float32,
                ) * score_scale
                column = block * vid + lax.broadcasted_iota(jnp.int32, (1, vid), 1)
                x = jnp.where(column < seen, x, LOW)
                scores[:, i * vid : (i + 1) * vid] = x
                wide = jnp.maximum(wide, lanes(x, jnp.maximum))
            new_best = jnp.maximum(best, jnp.max(wide, axis=1, keepdims=True))
            factor = jnp.exp2(best - new_best)
            weight, acc = weight * factor, acc * factor
            for i in range(per):
                w = jnp.exp2(scores[:, i * vid : (i + 1) * vid] - new_best)
                weight = weight + lanes(w, jnp.add)
                acc = acc + jnp.dot(
                    w.astype(jnp.bfloat16), vbuf[u * per + i, :, head_cols(h)],
                    preferred_element_type=jnp.float32,
                )
            return new_best, weight, acc

        state = (
            jnp.full((m_rows, 1), LOW, jnp.float32),
            jnp.zeros((m_rows, HD), jnp.float32),
            jnp.zeros((m_rows, HD), jnp.float32),
        )
        if n // per == 1:
            state = part(0, state)
        else:
            state = lax.fori_loop(0, n // per, part, state)
        _, weight, acc = state
        total = jnp.maximum(jnp.sum(weight, axis=1, keepdims=True), 1.0)
        result = jnp.where(seen > 0, acc / total, 0.0).astype(jnp.bfloat16)
        for g in range(GROUP):
            abuf[:, head_cols(h * GROUP + g)] = result[g * TBLK : (g + 1) * TBLK]

    def combine(c):
        wide = 512
        out_cols = pbuf.shape[2]

        def dest(j, carry):
            d = jnp.where(z < p // 2, p - 1 - j, j)

            def tile(t, carry):
                cols = pl.ds(pl.multiple_of(d * out_cols + t * wide, wide), wide)
                pbuf[c * p + d, :, pl.ds(pl.multiple_of(t * wide, wide), wide)] = jnp.dot(
                    abuf[...], wo[:, cols], preferred_element_type=jnp.float32
                )
                return carry

            lax.fori_loop(0, out_cols // wide, tile, 0)

            @pl.when((z == 0) & (d > 0))
            def _():
                sbuf[c * p + d] = pbuf[c * p + d].astype(jnp.bfloat16)
                sum_copy(c, d, True).start()

            @pl.when((z == p - 1) & (d < z))
            def _():
                sbuf[c * p + d] = pbuf[c * p + d].astype(jnp.bfloat16)
                sum_copy(c, d, False).start()

            return carry

        lax.fori_loop(0, p, dest, 0)

    def guarded(ok, f, *args):
        if isinstance(ok, bool):
            if ok:
                f(*args)
        else:
            pl.when(ok)(lambda: f(*args))

    text_own(0)
    kv_send(True, 0, 0)
    kv_send(False, 0, 0)
    for c in range(1, p):
        for h in range(c - 1, 0, -1):
            if c - 1 - h < chunks:
                text_hop(c - 1 - h, h)
        if c < min(chunks, p - 1):
            text_own(c)
        if c == min(2, p - 1) and bits:
            kv_step(0)

    def step(c, carry):
        @pl.when(c == 0)
        def _():
            local[0].wait()
            local[1].wait()

        text_hop(c, p - 1)
        project(c)
        for h in range(p - 2, 0, -1):
            guarded(c + p - 1 - h < chunks, text_hop, c + p - 1 - h, h)
        guarded(c + p - 1 < chunks, text_own, c + p - 1)

        @pl.when(c == 0)
        def _():
            for k in range(1, bits):
                kv_step(k)
            for copy in local[2:]:
                copy.wait()

        seen = visible_tokens(c)

        def head(h, carry):
            attend(c, h, seen)
            return carry

        lax.fori_loop(0, local_kv, head, 0)
        guarded(c - p + 1 >= 0, sum_last, c - p + 1)
        for h in range(p - 2, 0, -1):
            guarded(c - h >= 0, sum_hop, c - h, h)
        combine(c)
        return carry

    lax.fori_loop(0, chunks, step, 0)
    for k in range(p - 1):
        c = chunks + k
        for h in range(p - 1, 0, -1):
            if 0 <= c - h < chunks:
                sum_last(c - h) if h == p - 1 else sum_hop(c - h, h)

    for keys, order in ((True, key_order), (False, value_order)):
        for step_no in range(bits):
            for mask in masks_before(order, step_no):
                kv_copy(keys, mask, order[step_no]).wait_send()

    def drain(c, carry):
        for d in range(p):
            @pl.when((d <= z) & has_up)
            def _():
                text_copy(c, d, True).wait_send()

            @pl.when((d >= z) & has_dn)
            def _():
                text_copy(c, d, False).wait_send()

            @pl.when(d != z)
            def _():
                sum_copy(c, d, True).wait_send()
        return carry

    lax.fori_loop(0, chunks, drain, 0)


def solution(mesh):
    n, p = mesh.shape["seq"], mesh.shape["head"]

    def shards(text, wq, keys, values, wo, gate, lengths, limits):
        rows, feat = text.shape
        vid = keys.shape[0]
        chunks = rows // TBLK
        q_cols = wq.shape[1]
        out_cols = wo.shape[1] // p
        dma = pltpu.SemaphoreType.DMA
        any_spec = pl.BlockSpec(memory_space=pl.ANY)
        smem = pl.BlockSpec(memory_space=pltpu.SMEM)
        bf16, f32 = jnp.bfloat16, jnp.float32
        return pl.pallas_call(
            functools.partial(kernel, n, p),
            out_shape=jax.ShapeDtypeStruct((rows, out_cols), bf16),
            in_specs=[any_spec] * 5 + [smem] * 3,
            out_specs=pl.BlockSpec(memory_space=pltpu.VMEM),
            scratch_shapes=[
                pltpu.VMEM((p, rows, feat), bf16),
                pltpu.VMEM(wq.shape, bf16),
                pltpu.VMEM(wo.shape, bf16),
                pltpu.VMEM((n,) + keys.shape, bf16),
                pltpu.VMEM((n,) + values.shape, bf16),
                pltpu.VMEM((TBLK, q_cols), bf16),
                pltpu.VMEM((TBLK, q_cols), bf16),
                pltpu.VMEM((GROUP * TBLK, min(n * vid, max(vid, SUPER))), f32),
                pltpu.VMEM((chunks * p, TBLK, out_cols), f32),
                pltpu.VMEM((chunks * p, TBLK, out_cols), bf16),
                pltpu.VMEM((chunks * p, TBLK, out_cols), bf16),
                pltpu.VMEM((chunks * p, TBLK, out_cols), bf16),
                dma((5,)),
                dma((chunks * p,)), dma((chunks * p,)), dma((chunks * p,)),
                dma((chunks * p,)), dma((chunks * p,)), dma((chunks * p,)),
                dma((n,)), dma((n,)), dma((n,)), dma((n,)),
            ],
            compiler_params=pltpu.CompilerParams(
                collective_id=0, has_side_effects=True, vmem_limit_bytes=67043328
            ),
        )(text, wq, keys, values, wo, gate, lengths, limits)

    in_specs = (
        P("seq", "head"), P(None, "head"), P("seq", "head"), P("seq", "head"),
        P("head", None), P(), P(), P(),
    )
    return jax.shard_map(
        shards, mesh=mesh, in_specs=in_specs, out_specs=P("seq", "head"), check_vma=False
    )
```

```python
import functools
import math

import jax
import jax.numpy as jnp
from jax import lax
from jax.experimental import pallas as pl
from jax.experimental.pallas import tpu as pltpu
from jax.sharding import PartitionSpec as P

HD = 128
TBLK = 64
GROUP = 4
SUPER = 4096
LOW = -1e30


def kernel(
    n, p, text, wq_hbm, k_hbm, v_hbm, wo_hbm, gate, lengths, limits, out,
    tbuf, wq, wo, kbuf, vbuf, qbuf, abuf, scores, pbuf, sbuf, rup, rdn,
    local_sem, t_recv, t_up, t_dn, r_up, r_dn, r_send, k_recv, k_send, v_recv, v_send,
):
    s = lax.axis_index("seq")
    z = lax.axis_index("head")
    rows, feat = text.shape
    chunks = rows // TBLK
    vid = k_hbm.shape[0]
    local_kv = k_hbm.shape[1] // HD
    bits = n.bit_length() - 1

    def flip(index, mask):
        for b in range(bits):
            bit = 1 << b
            if mask & bit:
                index = index + bit - 2 * bit * ((index // bit) % 2)
        return index

    key_order = [*range(1, bits), 0]
    value_order = [*range(2, bits), 1, 0] if bits > 1 else [0]

    barrier = pltpu.get_barrier_semaphore()
    has_up, has_dn = z < p - 1, z > 0
    for b in range(bits):
        pl.semaphore_signal(barrier, inc=1, device_id={"seq": flip(s, 1 << b)})

    @pl.when(has_up)
    def _():
        pl.semaphore_signal(barrier, inc=1, device_id={"head": z + 1})

    @pl.when(has_dn)
    def _():
        pl.semaphore_signal(barrier, inc=1, device_id={"head": z - 1})

    local = [
        pltpu.make_async_copy(text, tbuf.at[z], local_sem.at[0]),
        pltpu.make_async_copy(wq_hbm, wq, local_sem.at[1]),
        pltpu.make_async_copy(k_hbm, kbuf.at[s], local_sem.at[2]),
        pltpu.make_async_copy(v_hbm, vbuf.at[s], local_sem.at[3]),
        pltpu.make_async_copy(wo_hbm, wo, local_sem.at[4]),
    ]
    for copy in local:
        copy.start()
    peers = bits + jnp.where(has_up, 1, 0) + jnp.where(has_dn, 1, 0)
    pl.semaphore_wait(barrier, peers)

    def span(c):
        return pl.ds(pl.multiple_of(c * TBLK, TBLK), TBLK)

    def text_copy(c, source, up, own=False):
        block = tbuf.at[source, span(c)]
        return pltpu.make_async_remote_copy(
            src_ref=text.at[span(c)] if own else block,
            dst_ref=block,
            send_sem=(t_up if up else t_dn).at[c * p + source],
            recv_sem=t_recv.at[c * p + source],
            device_id={"head": z + 1 if up else z - 1},
        )

    def text_own(c):
        @pl.when(has_up)
        def _():
            text_copy(c, z, True, True).start()

        @pl.when(has_dn)
        def _():
            text_copy(c, z, False, True).start()

    def text_hop(c, d):
        @pl.when(z - d >= 0)
        def _():
            text_copy(c, z - d, True).wait_recv()

            @pl.when(has_up)
            def _():
                text_copy(c, z - d, True).start()

        @pl.when(z + d < p)
        def _():
            text_copy(c, z + d, False).wait_recv()

            @pl.when(has_dn)
            def _():
                text_copy(c, z + d, False).start()

    def kv_copy(keys, mask, b):
        buf, hbm = (kbuf, k_hbm) if keys else (vbuf, v_hbm)
        recv, send = (k_recv, k_send) if keys else (v_recv, v_send)
        block = buf.at[flip(s, mask)]
        return pltpu.make_async_remote_copy(
            src_ref=hbm if mask == 0 else block,
            dst_ref=block,
            send_sem=send.at[mask | (1 << b)],
            recv_sem=recv.at[mask | (1 << b)],
            device_id={"seq": flip(s, 1 << b)},
        )

    def kv_send(keys, mask, step):
        order = key_order if keys else value_order
        for b in order[step:]:
            kv_copy(keys, mask, b).start()

    def kv_wait(keys, mask):
        buf, recv, send = (kbuf, k_recv, k_send) if keys else (vbuf, v_recv, v_send)
        block = buf.at[flip(s, mask)]
        pltpu.make_async_remote_copy(
            src_ref=block, dst_ref=block, send_sem=send.at[mask], recv_sem=recv.at[mask],
            device_id={"seq": flip(s, 1)},
        ).wait_recv()

    def masks_before(order, step):
        masks = [0]
        for b in order[:step]:
            masks = masks + [m | (1 << b) for m in masks]
        return masks

    def kv_step(step):
        for m_index in range(1 << step):
            for keys, order in ((True, key_order), (False, value_order)):
                mask = masks_before(order, step)[m_index] | (1 << order[step])
                kv_wait(keys, mask)
                kv_send(keys, mask, step + 1)

    def sum_copy(c, d, up):
        return pltpu.make_async_remote_copy(
            src_ref=sbuf.at[c * p + d],
            dst_ref=(rup if up else rdn).at[c * p + d],
            send_sem=r_send.at[c * p + d],
            recv_sem=(r_up if up else r_dn).at[c * p + d],
            device_id={"head": z + 1 if up else z - 1},
        )

    def sum_hop(c, h):
        for d in reversed(range(p)):
            @pl.when((z == h) & (z < d))
            def _():
                sum_copy(c, d, True).wait_recv()
                i = c * p + d
                sbuf[i] = (pbuf[i] + rup[i].astype(jnp.float32)).astype(jnp.bfloat16)
                sum_copy(c, d, True).start()
        for d in range(p):
            @pl.when((p - 1 - z == h) & (d < z))
            def _():
                sum_copy(c, d, False).wait_recv()
                i = c * p + d
                sbuf[i] = (pbuf[i] + rdn[i].astype(jnp.float32)).astype(jnp.bfloat16)
                sum_copy(c, d, False).start()

    def sum_last(c):
        i = c * p + z

        @pl.when(has_dn)
        def _():
            sum_copy(c, z, True).wait_recv()
            pbuf[i] = pbuf[i] + rup[i].astype(jnp.float32)

        @pl.when(has_up)
        def _():
            sum_copy(c, z, False).wait_recv()
            pbuf[i] = pbuf[i] + rdn[i].astype(jnp.float32)

        factor = jnp.tanh(jnp.full((1, out.shape[1]), gate[0], jnp.float32))
        out[span(c), :] = (factor * pbuf[i]).astype(jnp.bfloat16)

    def project(c):
        wide = 256

        def tile(j, carry):
            cols = pl.ds(pl.multiple_of(j * wide, wide), wide)
            total = jnp.zeros((TBLK, wide), jnp.float32)
            for source in range(p):
                total += jnp.dot(
                    tbuf[source, span(c), :], wq[source * feat : (source + 1) * feat, cols],
                    preferred_element_type=jnp.float32,
                )
            qbuf[:, cols] = total.astype(jnp.bfloat16)
            return carry

        lax.fori_loop(0, qbuf.shape[1] // wide, tile, 0)

    per = min(n, max(1, SUPER // vid))
    score_scale = math.log2(math.e) / math.sqrt(HD)

    def visible_tokens(c):
        limit = limits[s * chunks + c]
        total = jnp.int32(0)
        for f in range(lengths.shape[0]):
            total += jnp.where(f < limit, lengths[f], 0)
        return total

    def attend(seen):
        m_rows = GROUP * TBLK

        def lanes(x, op):
            parts = [x[:, i * HD : (i + 1) * HD] for i in range(x.shape[1] // HD)]
            return functools.reduce(op, parts)

        def score(h, block, i, wide):
            q = jnp.concatenate(
                [qbuf[:, (h * GROUP + g) * HD : (h * GROUP + g + 1) * HD] for g in range(GROUP)],
                axis=0,
            )
            x = lax.dot_general(
                q, kbuf[block, :, h * HD : (h + 1) * HD], (((1,), (1,)), ((), ())),
                preferred_element_type=jnp.float32,
            ) * score_scale
            column = block * vid + lax.broadcasted_iota(jnp.int32, (1, vid), 1)
            x = jnp.where(column < seen, x, LOW)
            scores[h % 2, :, i * vid : (i + 1) * vid] = x
            return jnp.maximum(wide, lanes(x, jnp.maximum))

        def part(u, states):
            low = jnp.full((m_rows, HD), LOW, jnp.float32)
            wide = low
            for i in range(per):
                wide = score(0, u * per + i, i, wide)
            done = []
            for h in range(local_kv):
                best, weight, acc = states[h]
                new_best = jnp.maximum(best, jnp.max(wide, axis=1, keepdims=True))
                factor = jnp.exp2(best - new_best)
                weight, acc = weight * factor, acc * factor
                wide = low
                for i in range(per):
                    if h + 1 < local_kv:
                        wide = score(h + 1, u * per + i, i, wide)
                    w = jnp.exp2(scores[h % 2, :, i * vid : (i + 1) * vid] - new_best)
                    weight = weight + lanes(w, jnp.add)
                    acc = acc + jnp.dot(
                        w.astype(jnp.bfloat16), vbuf[u * per + i, :, h * HD : (h + 1) * HD],
                        preferred_element_type=jnp.float32,
                    )
                done.append((new_best, weight, acc))
            return tuple(done)

        states = (
            (
                jnp.full((m_rows, 1), LOW, jnp.float32),
                jnp.zeros((m_rows, HD), jnp.float32),
                jnp.zeros((m_rows, HD), jnp.float32),
            ),
        ) * local_kv
        if n // per == 1:
            states = part(0, states)
        else:
            states = lax.fori_loop(0, n // per, part, states)
        for h in range(local_kv):
            _, weight, acc = states[h]
            total = jnp.maximum(jnp.sum(weight, axis=1, keepdims=True), 1.0)
            result = jnp.where(seen > 0, acc / total, 0.0).astype(jnp.bfloat16)
            for g in range(GROUP):
                head = h * GROUP + g
                abuf[:, head * HD : (head + 1) * HD] = result[g * TBLK : (g + 1) * TBLK]

    def combine(c):
        wide = 512
        out_cols = pbuf.shape[2]

        def dest(j, carry):
            d = jnp.where(z < p // 2, p - 1 - j, j)

            def tile(t, carry):
                cols = pl.ds(pl.multiple_of(d * out_cols + t * wide, wide), wide)
                pbuf[c * p + d, :, pl.ds(pl.multiple_of(t * wide, wide), wide)] = jnp.dot(
                    abuf[...], wo[:, cols], preferred_element_type=jnp.float32
                )
                return carry

            lax.fori_loop(0, out_cols // wide, tile, 0)

            @pl.when((z == 0) & (d > 0))
            def _():
                sbuf[c * p + d] = pbuf[c * p + d].astype(jnp.bfloat16)
                sum_copy(c, d, True).start()

            @pl.when((z == p - 1) & (d < z))
            def _():
                sbuf[c * p + d] = pbuf[c * p + d].astype(jnp.bfloat16)
                sum_copy(c, d, False).start()

            return carry

        lax.fori_loop(0, p, dest, 0)

    def guarded(ok, f, *args):
        if isinstance(ok, bool):
            if ok:
                f(*args)
        else:
            pl.when(ok)(lambda: f(*args))

    text_own(0)
    kv_send(True, 0, 0)
    kv_send(False, 0, 0)
    for c in range(1, p):
        for h in range(c - 1, 0, -1):
            if c - 1 - h < chunks:
                text_hop(c - 1 - h, h)
        if c < min(chunks, p - 1):
            text_own(c)
        if c == min(2, p - 1) and bits:
            kv_step(0)

    def step(c, carry):
        @pl.when(c == 0)
        def _():
            local[0].wait()
            local[1].wait()

        text_hop(c, p - 1)
        project(c)
        for h in range(p - 2, 0, -1):
            guarded(c + p - 1 - h < chunks, text_hop, c + p - 1 - h, h)
        guarded(c + p - 1 < chunks, text_own, c + p - 1)

        @pl.when(c == 0)
        def _():
            for k in range(1, bits):
                kv_step(k)
            for copy in local[2:]:
                copy.wait()

        seen = visible_tokens(c)

        attend(seen)
        guarded(c - p + 1 >= 0, sum_last, c - p + 1)
        for h in range(p - 2, 0, -1):
            guarded(c - h >= 0, sum_hop, c - h, h)
        combine(c)
        return carry

    lax.fori_loop(0, chunks, step, 0)
    for k in range(p - 1):
        c = chunks + k
        for h in range(p - 1, 0, -1):
            if 0 <= c - h < chunks:
                sum_last(c - h) if h == p - 1 else sum_hop(c - h, h)

    for keys, order in ((True, key_order), (False, value_order)):
        for step_no in range(bits):
            for mask in masks_before(order, step_no):
                kv_copy(keys, mask, order[step_no]).wait_send()

    def drain(c, carry):
        for d in range(p):
            @pl.when((d <= z) & has_up)
            def _():
                text_copy(c, d, True).wait_send()

            @pl.when((d >= z) & has_dn)
            def _():
                text_copy(c, d, False).wait_send()

            @pl.when(d != z)
            def _():
                sum_copy(c, d, True).wait_send()
        return carry

    lax.fori_loop(0, chunks, drain, 0)


def solution(mesh):
    n, p = mesh.shape["seq"], mesh.shape["head"]

    def shards(text, wq, keys, values, wo, gate, lengths, limits):
        rows, feat = text.shape
        vid = keys.shape[0]
        chunks = rows // TBLK
        q_cols = wq.shape[1]
        out_cols = wo.shape[1] // p
        dma = pltpu.SemaphoreType.DMA
        any_spec = pl.BlockSpec(memory_space=pl.ANY)
        smem = pl.BlockSpec(memory_space=pltpu.SMEM)
        bf16, f32 = jnp.bfloat16, jnp.float32
        return pl.pallas_call(
            functools.partial(kernel, n, p),
            out_shape=jax.ShapeDtypeStruct((rows, out_cols), bf16),
            in_specs=[any_spec] * 5 + [smem] * 3,
            out_specs=pl.BlockSpec(memory_space=pltpu.VMEM),
            scratch_shapes=[
                pltpu.VMEM((p, rows, feat), bf16),
                pltpu.VMEM(wq.shape, bf16),
                pltpu.VMEM(wo.shape, bf16),
                pltpu.VMEM((n,) + keys.shape, bf16),
                pltpu.VMEM((n,) + values.shape, bf16),
                pltpu.VMEM((TBLK, q_cols), bf16),
                pltpu.VMEM((TBLK, q_cols), bf16),
                pltpu.VMEM((2, GROUP * TBLK, min(n * vid, max(vid, SUPER))), f32),
                pltpu.VMEM((chunks * p, TBLK, out_cols), f32),
                pltpu.VMEM((chunks * p, TBLK, out_cols), bf16),
                pltpu.VMEM((chunks * p, TBLK, out_cols), bf16),
                pltpu.VMEM((chunks * p, TBLK, out_cols), bf16),
                dma((5,)),
                dma((chunks * p,)), dma((chunks * p,)), dma((chunks * p,)),
                dma((chunks * p,)), dma((chunks * p,)), dma((chunks * p,)),
                dma((n,)), dma((n,)), dma((n,)), dma((n,)),
            ],
            compiler_params=pltpu.CompilerParams(
                collective_id=0, has_side_effects=True, vmem_limit_bytes=67043328
            ),
        )(text, wq, keys, values, wo, gate, lengths, limits)

    in_specs = (
        P("seq", "head"), P(None, "head"), P("seq", "head"), P("seq", "head"),
        P("head", None), P(), P(), P(),
    )
    return jax.shard_map(
        shards, mesh=mesh, in_specs=in_specs, out_specs=P("seq", "head"), check_vma=False
    )
```
